256 devices in a mesh: gx: 16 (over x_hi, y, core), vert: 16 (over z, x_lo).
Axes of the slice: x: 4 (x_hi: 2, x_lo: 2; x = x_hi * 2 + x_lo), y: 4, z: 8, core: 2. Of those that a mesh axis runs over, the one named last changes fastest.
Arguments:
- dist: float32 [13824, 64, 256], P('vert', 'gx'), as said below
- offset: int32 [13824], P('vert'), may hold values from -6 to 6, as said below
- fraction: float32 [13824], P('vert'), may hold values from 0 to 1
- cross_velocity: float32 [2, 13824], P(None, 'vert'), may hold values from -4 to 4
- relax: float32 [64, 256], P('gx'), may hold values from 0.3 to 0.9
Outputs:
- updated: float32 [13824, 64, 256], P('vert', 'gx')
The draws below stay inside these ranges and needn't reach their ends.
Inputs may be any that keep to these rules, and one draw needn't show every extreme that they name: `offset`: each value from -6 to 6 inclusive; both ends are taken by some velocity. `dist`: Positive.
All inputs are finite; a program needn't handle non-finite values.
Results may differ from the reference program's by a relative error of at most 0.0003.
Values sent between devices are 32-bit elements; how exact they have to be, the bound alone decides.
No kernel may reach another device: no remote copies, remote signals or barrier semaphores. Data moves between devices by JAX's collectives and lax.ppermute only.
A program may use at most 64 MiB of HBM per device.

```python
import jax
import jax.numpy as jnp
from jax import lax

NV = 13824
MAXS = 6
NYZ = 256
NX = 64


def draw_dist(key, part):
    growth = 1.0 + 2.0 * jnp.arange(NV, dtype=jnp.float32) / (NV - 1)
    random_part = jnp.exp(jax.random.uniform(key, (NV, NX, NYZ), jnp.float32, jnp.log(0.5), jnp.log(2.0)))
    return random_part * growth[:, None, None]


def draw_offset(key, part):
    first, second, third = jax.random.split(jax.random.fold_in(key, 7), 3)
    values = jax.random.randint(first, (NV,), -MAXS, MAXS + 1, dtype=jnp.int32)
    upper_at = jax.random.randint(second, (), 0, NV, dtype=jnp.int32)
    lower_at = jnp.mod(upper_at + jax.random.randint(third, (), 1, NV, dtype=jnp.int32), NV)
    values = values.at[upper_at].set(MAXS)
    values = values.at[lower_at].set(-MAXS)
    return values


def levels(own_key, dims, pieces, low, high):
    factor_of = 1.0
    for dim, blocks in pieces:
        steps = jax.random.uniform(jax.random.fold_in(jax.random.fold_in(own_key, 6), dim), (blocks,), jnp.float32, low / len(pieces), high / len(pieces))
        factor_of = factor_of * jnp.repeat(jnp.exp(steps), dims[dim] // blocks).reshape((-1,) + (1,) * (len(dims) - 1 - dim))
    return factor_of


def gaussian(own_key, extent, scale, reach, cuts=(), held_as=jnp.bfloat16):
    gain = levels(own_key, extent, cuts, -0.22, 0.18) if cuts else 1.0
    array = jax.random.normal(own_key, extent, jnp.float32) * scale * gain
    return jnp.minimum(jnp.maximum(array, -reach), reach).astype(held_as)


def setup_inputs(seed: int = 0) -> dict:
    streams_of = jax.random.split(jax.random.key(seed), 6)
    return {
        "dist": draw_dist(jax.random.fold_in(streams_of[5], 71), 0),
        "offset": draw_offset(jax.random.fold_in(streams_of[5], 71), 0),
        "fraction": jnp.clip(1.0 * jax.random.uniform(streams_of[2], (NV,), jnp.float32) ** levels(streams_of[2], (NV,), ((0, 16),), -0.2, 0.2), 0.0, 1.0),
        "cross_velocity": gaussian(streams_of[3], (2, NV), 1.5, 4.0, ((1, 16),), jnp.float32),
        "relax": jnp.clip(0.3 + 0.59999996 * jax.random.uniform(streams_of[4], (NX, NYZ), jnp.float32) ** levels(streams_of[4], (NX, NYZ), ((0, 16),), -0.2, 0.2), 0.3, 0.9),
    }


def stencil_matrix(offset, fraction, row_count, col_count, anchor):
    position = 1.0 - fraction
    weights = jnp.stack([
        -position * (position - 1.0) * (position - 2.0) / 6.0,
        (position + 1.0) * (position - 1.0) * (position - 2.0) / 2.0,
        -(position + 1.0) * position * (position - 2.0) / 2.0,
        (position + 1.0) * position * (position - 1.0) / 6.0], axis=1)
    row_index = jnp.arange(row_count, dtype=jnp.int32)
    tap_index = jnp.arange(4, dtype=jnp.int32)
    target = jnp.mod(row_index[None, :, None] - offset.astype(jnp.int32)[:, None, None] - 2 + tap_index[None, None, :] + anchor, col_count)
    onehot = (target[..., None] == jnp.arange(col_count, dtype=jnp.int32)).astype(weights.dtype)
    return jnp.einsum('vrjc,vj->vrc', onehot, weights, precision=lax.Precision.HIGHEST)


def velocities(offset, fraction, cross_velocity):
    along = (offset.astype(fraction.dtype) + fraction) * (3.0 / MAXS)
    return along, cross_velocity[0], cross_velocity[1]


def cell_state(sums):
    density = sums[0]
    mean_x = sums[1] / density
    mean_y = sums[2] / density
    mean_z = sums[3] / density
    temper = (sums[4] / density - (mean_x * mean_x + mean_y * mean_y + mean_z * mean_z)) / 3.0
    return jnp.stack([density, mean_x, mean_y, mean_z, temper])


def equilibrium(vel_x, vel_y, vel_z, state):
    diff_x = vel_x[:, None, None] - state[1]
    diff_y = vel_y[:, None, None] - state[2]
    diff_z = vel_z[:, None, None] - state[3]
    return jnp.exp(-(diff_x * diff_x + diff_y * diff_y + diff_z * diff_z) / (2.0 * state[4]))


def reference(dist, offset, fraction, cross_velocity, relax):
    blocks = NV // 128

    def advect(inputs):
        field, shift_block, frac_block = inputs
        matrix = stencil_matrix(shift_block, frac_block, NX, NX, 0)
        return jnp.einsum('vrc,vcn->vrn', matrix, field, precision=lax.Precision.HIGHEST)

    shifted = lax.map(advect, (dist.reshape(blocks, 128, NX, NYZ), offset.reshape(blocks, 128), fraction.reshape(blocks, 128)))
    shifted = shifted.reshape(NV, NX, NYZ)
    vel_x, vel_y, vel_z = velocities(offset, fraction, cross_velocity)
    coeffs = jnp.stack([jnp.ones_like(vel_x), vel_x, vel_y, vel_z, vel_x * vel_x + vel_y * vel_y + vel_z * vel_z])
    sums = jnp.einsum('mv,vxn->mxn', coeffs, shifted, precision=lax.Precision.HIGHEST)
    state = cell_state(sums)
    vel_blocks = (vel_x.reshape(blocks, 128), vel_y.reshape(blocks, 128), vel_z.reshape(blocks, 128))

    def accumulate(carry, inputs):
        return carry + jnp.sum(equilibrium(inputs[0], inputs[1], inputs[2], state), axis=0), None

    total, _ = lax.scan(accumulate, jnp.zeros((NX, NYZ), dtype=shifted.dtype), vel_blocks)

    def finish(inputs):
        field, part_x, part_y, part_z = inputs
        weight = equilibrium(part_x, part_y, part_z, state)
        return field + relax[None] * (state[0] * weight / total - field)

    updated = lax.map(finish, (shifted.reshape(blocks, 128, NX, NYZ),) + vel_blocks)
    return updated.reshape(NV, NX, NYZ)
```

```python
import jax
import jax.numpy as jnp
from jax import lax
from jax.experimental import pallas as pl
from jax.experimental.pallas import tpu as pltpu
from jax.sharding import Mesh
from jax.sharding import PartitionSpec as P

MAXS = 6
CLASSES = 2 * MAXS + 1
GX = ("gx_0", "gx_1", "gx_2")
LOG2E = 1.4426950408889634

NEED = {
    b: [
        [c for c in range(CLASSES) if -(c - MAXS) - 2 <= 4 * b + y <= 4 - (c - MAXS)]
        for y in range(4)
    ]
    for b in (-2, -1, 1, 2)
}
BLOCKS = (-2, -1, 1, 2)
SHARE = {-2: 1.0, -1: 2.27, 1: 2.03, 2: 0.63}


def room(block, group_count):
    return int(SHARE[block] * group_count)


def spans(block):
    return [(y, cs[0], cs[-1] + 1) for y, cs in enumerate(NEED[block]) if cs]


def rank_kernel(offset_ref, pos_ref, starts_ref):
    rows, lanes = offset_ref.shape
    count = CLASSES * rows
    cls = offset_ref[...] + MAXS
    member = jnp.concatenate([(cls == c).astype(jnp.float32) for c in range(CLASSES)], axis=0)

    def dot(a, b):
        return lax.dot(a, b, precision=lax.Precision.HIGHEST, preferred_element_type=jnp.float32)

    def grid(shape, dim):
        return lax.broadcasted_iota(jnp.int32, shape, dim)

    square = (lanes, lanes)
    upto = (grid(square, 0) <= grid(square, 1)).astype(jnp.float32)
    prefix = dot(member, upto)
    total = dot(member, jnp.ones(square, jnp.float32))
    square = (count, count)
    row, col = grid(square, 0), grid(square, 1)
    shift = rows.bit_length() - 1
    row_class, col_class = lax.shift_right_logical(row, shift), lax.shift_right_logical(col, shift)
    same = row_class == col_class
    before = dot((same & (col < row)).astype(jnp.float32), total)
    members = dot(same.astype(jnp.float32), total)
    groups = jnp.floor((members + 7.0) * 0.125)
    start = dot((col_class < row_class).astype(jnp.float32) * (8.0 / rows), groups)
    where = member * (prefix + before + start - 1.0)
    pos = where[:rows]
    for c in range(1, CLASSES):
        pos = pos + where[c * rows : (c + 1) * rows]
    pos_ref[...] = pos.astype(jnp.int32)
    wide = (starts_ref.shape[0], count)
    ahead = (lax.shift_right_logical(grid(wide, 1), shift) < grid(wide, 0)).astype(jnp.float32)
    starts_ref[...] = dot(ahead * (1.0 / rows), groups).astype(jnp.int32)


def ranked(offset):
    rows = 8
    lanes = offset.shape[0] // rows
    return pl.pallas_call(
        rank_kernel,
        out_shape=(
            jax.ShapeDtypeStruct((rows, lanes), jnp.int32),
            jax.ShapeDtypeStruct((16, lanes), jnp.int32),
        ),
        name="rank",
    )(offset.reshape(rows, lanes))


def pack_kernel(pos_ref, starts_ref, field_ref, sorted_ref, *sent):
    rows, lanes = pos_ref.shape
    for r in range(rows):

        def place(lane, _):
            to = pl.multiple_of(pos_ref[r, lane] * 8, 8)
            sorted_ref[pl.ds(to, 8), :] = field_ref[r * lanes + lane]
            return 0

        lax.fori_loop(0, lanes, place, 0, unroll=4)
    for block, buffer in zip(BLOCKS, sent):
        cap = buffer.shape[0] // 16
        slot = 0
        for y, first, last in spans(block):
            low, high = starts_ref[first, 0], starts_ref[last, 0]
            length = jnp.maximum(jnp.minimum(high - low, cap - slot), 0)

            def copy(i, _):
                for h in range(2):
                    to = pl.multiple_of((slot + i) * 16 + h * 8, 8)
                    buffer[pl.ds(to, 8), :] = sorted_ref[
                        pl.ds((low + i) * 64 + h * 4 + y, 8, stride=8), :
                    ]
                return 0

            lax.fori_loop(0, length, copy, 0)
            slot = slot + length


def packed(pos, starts, field, group_count):
    padded = (group_count + CLASSES) * 64
    shapes = [(padded, 128)] + [(room(b, group_count) * 16, 128) for b in BLOCKS]
    vmem = pl.BlockSpec(memory_space=pltpu.VMEM)
    smem = pl.BlockSpec(memory_space=pltpu.SMEM)
    return pl.pallas_call(
        pack_kernel,
        out_shape=[jax.ShapeDtypeStruct(s, jnp.float32) for s in shapes],
        in_specs=[smem, smem, vmem],
        out_specs=[vmem] * len(shapes),
        compiler_params=pltpu.CompilerParams(vmem_limit_bytes=40 * 2**20),
        cost_estimate=pl.CostEstimate(flops=3_000_000, bytes_accessed=12_000_000, transcendentals=0),
        name="pack",
    )(pos, starts, field)


def finish_kernel(pos_ref, starts_ref, own, left2, left1, right1, right2, param_ref, state_ref, out_ref, wide, moved):
    received = {-2: left2, -1: left1, 1: right1, 2: right2}
    for q in range(6):
        for r in range(8):
            wide[pl.ds((q * 8 + r) * 8, 8), :] = jnp.broadcast_to(state_ref[q, r : r + 1, :], (8, 128))
    base = {}
    for block in BLOCKS:
        cap = received[block].shape[0] // 16
        slot = 0
        for y, first, last in spans(block):
            low, high = starts_ref[first, 0], starts_ref[last, 0]
            base[block, y] = (slot - low, cap - 1)
            slot = slot + (high - low)

    def cell(block, y, h, group):
        if block == 0:
            return own[pl.ds(group * 64 + h * 4 + y, 8, stride=8), :]
        shift, last = base[block, y]
        at = jnp.minimum(group + shift, last)
        return received[block][pl.ds(pl.multiple_of(at * 16 + h * 8, 8), 8), :]

    for c in range(CLASSES):
        first_cell = -(c - MAXS) - 2

        def advance(group, _):
            param = param_ref[pl.ds(pl.multiple_of(group * 8, 8), 8), :]
            w0, w1, w2, w3, vx, vy, vz = [
                jnp.broadcast_to(param[:, j : j + 1], (8, 128)) for j in range(7)
            ]
            for h in range(2):
                window = [
                    cell((first_cell + o) // 4, (first_cell + o) % 4, h, group) for o in range(7)
                ]
                for x in range(4):
                    r = h * 4 + x
                    ux, uy, uz, scale, gain, keep = [
                        wide[pl.ds((q * 8 + r) * 8, 8), :] for q in range(6)
                    ]
                    shifted = (
                        w0 * window[x] + w1 * window[x + 1] + w2 * window[x + 2] + w3 * window[x + 3]
                    )
                    dx, dy, dz = vx - ux, vy - uy, vz - uz
                    weight = jnp.exp((dx * dx + dy * dy + dz * dz) * scale)
                    moved[pl.ds(group * 64 + r, 8, stride=8), :] = keep * shifted + gain * weight
            return 0

        lax.fori_loop(starts_ref[c, 0], starts_ref[c + 1, 0], advance, 0)
    rows, lanes = pos_ref.shape
    for r in range(rows):

        def place(lane, _):
            at = pl.multiple_of(pos_ref[r, lane] * 8, 8)
            out_ref[r * lanes + lane] = moved[pl.ds(at, 8), :]
            return 0

        lax.fori_loop(0, lanes, place, 0, unroll=4)


def finished(pos, starts, own, received, param, state, count):
    vmem = pl.BlockSpec(memory_space=pltpu.VMEM)
    smem = pl.BlockSpec(memory_space=pltpu.SMEM)
    return pl.pallas_call(
        finish_kernel,
        out_shape=jax.ShapeDtypeStruct((count, 8, 128), jnp.float32),
        in_specs=[smem, smem] + [vmem] * 7,
        out_specs=vmem,
        scratch_shapes=[pltpu.VMEM((6 * 64, 128), jnp.float32), pltpu.VMEM(own.shape, jnp.float32)],
        compiler_params=pltpu.CompilerParams(vmem_limit_bytes=48 * 2**20),
        cost_estimate=pl.CostEstimate(flops=25_000_000, bytes_accessed=14_000_000, transcendentals=900_000),
        name="finish",
    )(pos, starts, own, *received, param, state)


def sent_to_all(array, axis):
    copies = jnp.broadcast_to(array, (lax.axis_size(axis), *array.shape))
    return lax.all_to_all(copies, axis, split_axis=0, concat_axis=0, tiled=True)


def of_everyone(array, axis):
    return sent_to_all(array, axis).sum(axis=0)


def along_line(array, step):
    size = lax.axis_size(GX)
    return lax.ppermute(array, GX, [(i, (i + step) % size) for i in range(size)])


def lagrange(fraction):
    t = 1.0 - fraction
    return [
        -t * (t - 1.0) * (t - 2.0) / 6.0,
        (t + 1.0) * (t - 1.0) * (t - 2.0) / 2.0,
        -(t + 1.0) * t * (t - 2.0) / 2.0,
        (t + 1.0) * t * (t - 1.0) / 6.0,
    ]


def cell_state(sums):
    density = sums[0]
    mean_x = sums[1] / density
    mean_y = sums[2] / density
    mean_z = sums[3] / density
    temper = (sums[4] / density - (mean_x * mean_x + mean_y * mean_y + mean_z * mean_z)) / 3.0
    return density, mean_x, mean_y, mean_z, temper


def moments(field, offset, weights, coeffs):
    reach = jnp.arange(-MAXS - 1, MAXS + 3, dtype=jnp.int32)
    stencil = sum(
        jnp.where(offset[None, :] + 2 - j == reach[:, None], weights[j][None, :], 0.0) for j in range(4)
    )
    table = coeffs[:, None, :] * stencil[None]
    spread = jnp.einsum("mdv,vrl->mdrl", table, field, precision=lax.Precision.HIGHEST)
    spread = spread.reshape(5, len(reach), 2, 4, 128)
    parts = {}
    for block in (-2, -1, 0, 1, 2):
        cells = []
        for x in range(4):
            terms = [
                spread[:, x + 4 * block - y + MAXS + 1, :, y]
                for y in range(4)
                if 0 <= x + 4 * block - y + MAXS + 1 < len(reach)
            ]
            cells.append(sum(terms) if terms else jnp.zeros((5, 2, 128), jnp.float32))
        parts[block] = jnp.stack(cells, axis=2).reshape(5, 8, 128)
    return parts


def everything(dist, offset, weights):
    window = jnp.concatenate(
        [along_line(dist, 2), along_line(dist, 1), dist, along_line(dist, -1), along_line(dist, -2)], axis=1
    )
    cell = jnp.arange(4, dtype=jnp.int32)[:, None, None]
    tap = jnp.arange(4, dtype=jnp.int32)[None, :, None]
    column = jnp.arange(20, dtype=jnp.int32)[None, None, :]
    hit = (cell + tap - 2 + 8 - offset[:, None, None, None] == column).astype(jnp.float32)
    matrix = jnp.einsum("vrjc,vj->vrc", hit, jnp.stack(weights, axis=1), precision=lax.Precision.HIGHEST)
    return jnp.einsum("vrc,vcn->vrn", matrix, window, precision=lax.Precision.HIGHEST)


def by_half(array):
    lead = array.shape[:-2]
    return jnp.moveaxis(array.reshape(*lead, 4, 2, 128), -2, -3).reshape(*lead, 8, 128)


def by_cell(array):
    lead = array.shape[:-2]
    return jnp.moveaxis(array.reshape(*lead, 2, 4, 128), -3, -2).reshape(*lead, 4, 256)


def per_device(dist, offset, fraction, cross_velocity, relax):
    count = dist.shape[0]
    group_count = count // 8
    field = by_half(dist)
    pos, starts = ranked(offset)
    own, *sent = packed(pos, starts, field, group_count)
    received = [along_line(buffer, -block) for block, buffer in zip(BLOCKS, sent)]

    weights = lagrange(fraction)
    vel_x = (offset.astype(fraction.dtype) + fraction) * (3.0 / MAXS)
    vel_y, vel_z = cross_velocity[0], cross_velocity[1]
    coeffs = jnp.stack(
        [jnp.ones_like(vel_x), vel_x, vel_y, vel_z, vel_x * vel_x + vel_y * vel_y + vel_z * vel_z]
    )
    parts = moments(field, offset, weights, coeffs)
    sums = parts[0] + sum(along_line(parts[b], b) for b in BLOCKS)
    density, mean_x, mean_y, mean_z, temper = cell_state(of_everyone(sums, "vert"))
    diff_x = vel_x[:, None, None] - mean_x
    diff_y = vel_y[:, None, None] - mean_y
    diff_z = vel_z[:, None, None] - mean_z
    scale = -1.0 / (2.0 * temper)
    weight = jnp.exp((diff_x * diff_x + diff_y * diff_y + diff_z * diff_z) * scale)
    begin = starts[:, 0]
    too_many = jnp.zeros((), jnp.bool_)
    for block in BLOCKS:
        length = sum(begin[last] - begin[first] for _, first, last in spans(block))
        too_many = too_many | (length > room(block, group_count))
    flag = jnp.full((1, 128), too_many.astype(jnp.float32))
    both = of_everyone(jnp.concatenate([jnp.sum(weight, axis=0), flag], axis=0), "vert")
    total = both[:8]
    share = by_half(relax)
    gain = share * density / total

    param = jnp.stack([*weights, vel_x, vel_y, vel_z, jnp.zeros_like(vel_x)], axis=1)
    slot = jnp.arange((group_count + CLASSES) * 8, dtype=jnp.int32)
    choose = (slot[:, None] == pos.reshape(-1)[None, :]).astype(jnp.float32)
    param = jnp.dot(choose, param, precision=lax.Precision.HIGHEST)
    state = jnp.stack([mean_x, mean_y, mean_z, scale, gain, 1.0 - share])

    def in_general(_):
        advected = by_half(everything(dist, offset, weights))
        return advected * (1.0 - share) + gain * weight_of_all()

    def weight_of_all():
        return jnp.exp((diff_x * diff_x + diff_y * diff_y + diff_z * diff_z) * scale)

    def in_room(_):
        return finished(pos, starts, own, received, param, state, count)

    return by_cell(lax.cond(both[8, 0] > 0.0, in_general, in_room, 0))


def solution(mesh):
    torus = Mesh(
        mesh.devices.reshape(2, 4, 2, mesh.shape["vert"]), ("gx_0", "gx_1", "gx_2", "vert")
    )
    placed = (P("vert", GX, None), P("vert"), P("vert"), P(None, "vert"), P(GX, None))
    return jax.shard_map(
        per_device, mesh=torus, in_specs=placed, out_specs=P("vert", GX, None), check_vma=False
    )
```
